256 devices in a mesh: rows: 64 (over z, y, core), mem: 4 (over x).
Axes of the slice: x: 4, y: 4, z: 8, core: 2. Of those that a mesh axis runs over, the one named last changes fastest.
Arguments:
- control: bfloat16 [16, 32, 2, 512, 512], P('mem', None, None, 'rows'), may hold values from -6 to 6
- vert_root: float32 [32, 32], replicated, may hold values from -1 to 1
- loc_spec: float32 [512], replicated, may hold values from 0.1 to 1
- legendre: bfloat16 [512, 512, 768], P('rows'), as said below
- wave_table: int32 [512], replicated, may hold values from 0 to 511, as said below
- lat_order: int32 [768], replicated, may hold values from 0 to 767, each once
- perturb: bfloat16 [768, 16, 32, 1536], P('rows', None, 'mem'), may hold values from -3 to 3
Outputs:
- increment: bfloat16 [768, 32, 1536], P('rows', 'mem')
The draws below stay inside these ranges and needn't reach their ends.
Inputs may be any that keep to these rules, and one draw needn't show every extreme that they name: `wave_table`: every zonal wavenumber 0 to 511 sits in exactly one slot; the slots held by one index of rows are pairs m and 511 - m. legendre[s, n, t] is zero where n < wave_table[s]. `lat_order`: a permutation.
All inputs are finite; a program needn't handle non-finite values.
Results may differ from the reference program's by a relative error of at most 0.0085.
Values may be sent and summed in bfloat16 or wider, within the bound.
A program may use at most 128 MiB of HBM per device.

```python
import math
import jax
import jax.numpy as jnp
from jax import lax

NM = 512
NT = 512
NLAT = 768
NLON = 1536
MEMBERS = 16
LEV = 32
N_ROWS = 64


def pair_table(key):
    subkey = jax.random.fold_in(key, 7)
    permuted = jax.random.permutation(subkey, NM // 2).astype(jnp.int32)
    lower_half = permuted.reshape(N_ROWS, NM // (2 * N_ROWS))
    return jnp.concatenate([lower_half, NM - 1 - lower_half], axis=1).reshape(NM).astype(jnp.int32)


def draw_wave_table(key, part):
    return pair_table(key)


def draw_legendre(key, part):
    table = pair_table(key)
    subkey = jax.random.fold_in(key, 11)
    values = jax.random.normal(subkey, (NM, NT, NLAT), jnp.float32)
    totals = jnp.arange(NT, dtype=jnp.int32)
    triangle = (totals[None, :] >= table[:, None]).astype(jnp.float32)
    factor = (4.0 * NM * NT) ** (-0.5)
    return (values * factor * triangle[:, :, None]).astype(jnp.bfloat16)


def block_levels(key, extent, split, low, top_value):
    level = 1.0
    for dim, shards_of in split:
        draws = jax.random.uniform(jax.random.fold_in(jax.random.fold_in(key, 6), dim), (shards_of,), jnp.float32, low / len(split), top_value / len(split))
        level = level * jnp.repeat(jnp.exp(draws), extent[dim] // shards_of).reshape((-1,) + (1,) * (len(extent) - 1 - dim))
    return level


def noise(rng, dims, spread, reach, pieces=(), held_as=jnp.bfloat16):
    gain = block_levels(rng, dims, pieces, -0.22, 0.18) if pieces else 1.0
    values = jax.random.normal(rng, dims, jnp.float32) * spread * gain
    return jnp.minimum(jnp.maximum(values, -reach), reach).astype(held_as)


def setup_inputs(seed: int = 0) -> dict:
    key_list = jax.random.split(jax.random.key(seed), 8)
    control = noise(key_list[0], (MEMBERS, LEV, 2, NM, NT), 1.0, 6.0, ((0, 4), (3, 64)))
    vert_root = noise(key_list[1], (LEV, LEV), LEV ** -0.5, 1.0, (), jnp.float32)
    loc_spec = jnp.clip(jnp.exp(jax.random.uniform(key_list[2], (NT,), jnp.float32, math.log(0.1), math.log(1.0))), 0.1, 1.0)
    legendre = draw_legendre(jax.random.fold_in(key_list[7], 71), 0)
    wave_table = draw_wave_table(jax.random.fold_in(key_list[7], 71), 0)
    lat_order = jax.random.permutation(key_list[5], NLAT).astype(jnp.int32)
    perturb = noise(key_list[6], (NLAT, MEMBERS, LEV, NLON), 0.5, 3.0, ((0, 64), (2, 4)))
    return {"control": control, "vert_root": vert_root, "loc_spec": loc_spec, "legendre": legendre, "wave_table": wave_table, "lat_order": lat_order, "perturb": perturb}


def make_basis(wave_table, lon_count):
    longitude = lax.iota(jnp.int32, lon_count)
    phases = (wave_table[:, None] * longitude[None, :]) % lon_count
    angles = phases.astype(jnp.float32) * (2.0 * math.pi / lon_count)
    weights = jnp.where(wave_table == 0, 1.0, 2.0).astype(jnp.float32)[:, None]
    return jnp.stack([weights * jnp.cos(angles), -weights * jnp.sin(angles)]).astype(jnp.bfloat16)


def reference(control, vert_root, loc_spec, legendre, wave_table, lat_order, perturb):
    scaled = control.astype(jnp.float32) * loc_spec
    spectra = jnp.einsum('lv,kvrsn->klrsn', vert_root, scaled, precision=lax.Precision.HIGHEST).astype(jnp.bfloat16)
    zonal_basis = make_basis(wave_table, NLON).astype(jnp.float32)
    legendre_wide = legendre.astype(jnp.float32)

    def one_level(level_index):
        level_spec = lax.dynamic_index_in_dim(spectra, level_index, 1, keepdims=False).astype(jnp.float32)
        fourier = jnp.einsum('snt,krsn->strk', legendre_wide, level_spec, precision=lax.Precision.HIGHEST).astype(jnp.bfloat16)
        fourier = jnp.take(fourier, lat_order, axis=1).astype(jnp.float32)
        fields = jnp.einsum('sjrk,rsx->jkx', fourier, zonal_basis, precision=lax.Precision.HIGHEST).astype(jnp.bfloat16)
        member_ptb = lax.dynamic_index_in_dim(perturb, level_index, 2, keepdims=False).astype(jnp.float32)
        return jnp.sum(fields.astype(jnp.float32) * member_ptb, axis=1).astype(jnp.bfloat16)

    stacked = lax.map(one_level, jnp.arange(LEV, dtype=jnp.int32))
    return jnp.transpose(stacked, (1, 0, 2))
```

```python
import functools
import math

import jax
import jax.numpy as jnp
from jax import lax
from jax.experimental import pallas as pl
from jax.experimental.pallas import tpu as pltpu
from jax.sharding import PartitionSpec as P

HALVES = 2
QUADS = 2
LATS = 4
LANES = 128
PIECE = 512
VMEM_LIMIT = 60 * 1024 * 1024
MESH = pl.DeviceIdType.MESH
Z, Y, CORES = 8, 4, 2


def f32(x):
    return x.astype(jnp.float32)


def bf16(x):
    return x.astype(jnp.bfloat16)


def iota(shape, dim):
    return lax.broadcasted_iota(jnp.int32, shape, dim)


def peer(rows, step):
    z, y, c = rows // (Y * CORES), (rows // CORES) % Y, rows % CORES
    k, w = step // (Y * CORES), step % (Y * CORES)
    dz = Z // 2 + (1 - 2 * (k % 2)) * ((k + 1) // 2)
    z = lax.rem(z + dz, Z)
    y = lax.rem(y + w // CORES + 1, Y)
    c = lax.rem(c + w + 1, CORES)
    return (z * Y + y) * CORES + c


def kernel(
    root_ref, loc_ref, order_ref, wave_ref, ctl_hbm, leg_hbm, ptb_hbm, out_ref,
    ctl, leg, ptb, kron, onehot, sx, rx, stage, sbuf, gbuf, basis, part,
    load_sem, xs_sem, xr_sem, as_sem, ar_sem, own_sem,
):
    rows = lax.axis_index("rows")
    me = lax.axis_index("mem")
    mem_count, row_count = 4, 64
    members, modes, _, slots, totals = ctl.shape
    taken = members // HALVES
    levels = modes // mem_count
    lat_count = leg.shape[2]
    quad = slots // QUADS
    tall = taken * levels

    barrier = pltpu.get_barrier_semaphore()

    def greet(step, carry):
        pl.semaphore_signal(barrier, inc=1, device_id=(peer(rows, step), me), device_id_type=MESH)
        return carry

    for i in range(1, mem_count):
        pl.semaphore_signal(
            barrier, inc=1, device_id=(rows, lax.rem(me + i, mem_count)), device_id_type=MESH
        )
    lax.fori_loop(0, row_count - 1, greet, 0)

    ctl_in = [
        pltpu.make_async_copy(
            ctl_hbm.at[pl.ds(h * taken, taken)], ctl.at[pl.ds(h * taken, taken)], load_sem.at[h]
        )
        for h in range(HALVES)
    ]
    leg_in = pltpu.make_async_copy(leg_hbm, leg, load_sem.at[2])
    ptb_in = pltpu.make_async_copy(ptb_hbm, ptb, load_sem.at[3])
    for c in ctl_in:
        c.start()
    leg_in.start()
    ptb_in.start()

    size = slots * taken * modes
    row, col = iota((size, modes), 0), iota((size, modes), 1)
    level = lax.rem(me + row // (slots * tall), mem_count) * levels + row % levels
    pick = bf16(f32(level == col))
    spread = bf16(f32(iota((modes, size), 0) == (iota((modes, size), 1) // slots) % modes))
    wide = jnp.dot(pick, bf16(root_ref[...]), preferred_element_type=jnp.float32)
    wide = jnp.dot(bf16(wide), spread, preferred_element_type=jnp.float32)
    row, col = iota((size, size), 0), iota((size, size), 1)
    same = ((row // tall) % slots == col % slots) & ((row // levels) % taken == col // (modes * slots))
    kron[...] = bf16(jnp.where(same, wide, 0.0))

    def spectra(h):
        ctl_in[h].wait()
        for r in range(2):
            x = f32(ctl[h * taken : (h + 1) * taken, :, r])
            x = bf16(x.reshape(taken * modes * slots, totals))
            spec = jnp.dot(kron[...], x, preferred_element_type=jnp.float32) * loc_ref[...]
            spec = bf16(spec).reshape(mem_count, slots, tall, totals)
            sx[h, :, :, r] = spec
            rx[h, 0, :, r] = spec[0]

    def exchange(h, q, i):
        part_of = pl.ds(q * quad, quad)
        return pltpu.make_async_remote_copy(
            src_ref=sx.at[h, i, part_of],
            dst_ref=rx.at[h, i, part_of],
            send_sem=xs_sem,
            recv_sem=xr_sem.at[h * QUADS + q],
            device_id=(rows, lax.rem(me + i, mem_count)),
            device_id_type=MESH,
        )

    spectra(0)
    pl.semaphore_wait(barrier, row_count + mem_count - 2)
    for q in range(QUADS):
        for i in range(1, mem_count):
            exchange(0, q, i).start()
    spectra(1)
    for q in range(QUADS):
        for i in range(1, mem_count):
            exchange(1, q, i).start()

    onehot[...] = bf16(f32(iota((lat_count, lat_count), 0) == order_ref[...])).T
    leg_in.wait()

    def wait_exchange(hq):
        h, q = hq // QUADS, hq % QUADS
        got = rx.at[h, pl.ds(1, mem_count - 1), pl.ds(q * quad, quad)]
        pltpu.make_async_copy(got, got, xr_sem.at[hq]).wait()

    def send(hq, b, dest, sem):
        lo, n = ((0, 32), (32, 16))[b]
        return pltpu.make_async_remote_copy(
            src_ref=sbuf.at[hq, dest, pl.ds(lo, n)],
            dst_ref=gbuf.at[hq, rows, pl.ds(lo, n)],
            send_sem=as_sem,
            recv_sem=sem,
            device_id=(dest, me),
            device_id_type=MESH,
        )

    def legendre_step(hq, carry):
        h, q = hq // QUADS, hq % QUADS
        wait_exchange(hq)
        for s in range(quad):
            x = rx[h, :, q * quad + s]
            x = jnp.concatenate([x[:, r].reshape(mem_count * tall, totals) for r in range(2)], axis=0)
            four = bf16(jnp.dot(x, leg[q * quad + s], preferred_element_type=jnp.float32))
            stage[pl.ds(s, lat_count, stride=quad), :] = lax.dot_general(
                onehot[...], four, (((1,), (1,)), ((), ())), preferred_element_type=jnp.float32
            )
        sbuf[hq] = bf16(stage[...]).reshape(row_count, lat_count * quad // row_count, LANES)
        pltpu.make_async_copy(sbuf.at[hq, rows], gbuf.at[hq, rows], own_sem).start()
        for b in range(2):
            def push(step, c):
                send(hq, b, peer(rows, step), ar_sem.at[hq * 2 + b]).start()
                return c
            lax.fori_loop(0, row_count - 1, push, 0)
        return carry

    lax.fori_loop(0, HALVES * QUADS, legendre_step, 0)

    slot_count, lon_count = basis.shape[0] // 2, basis.shape[1]
    wave = jnp.broadcast_to(wave_ref[...], (LANES, slot_count)).T
    weight = jnp.where(wave == 0, 1.0, 2.0)
    angle = f32(lax.rem(wave * iota((slot_count, LANES), 1), lon_count)) * (2.0 * math.pi / lon_count)
    fine_cos, fine_sin = weight * jnp.cos(angle), weight * jnp.sin(angle)
    turns = lon_count // LANES
    angle = f32(lax.rem(wave * iota((slot_count, LANES), 1), turns)) * (2.0 * math.pi / turns)
    wide_cos, wide_sin = jnp.cos(angle), jnp.sin(angle)
    for a in range(turns):
        x = pl.ds(a * LANES, LANES)
        wc = wide_cos[:, a : a + 1]
        ws = wide_sin[:, a : a + 1]
        basis[pl.ds(0, slot_count), x] = bf16(fine_cos * wc - fine_sin * ws)
        basis[pl.ds(slot_count, slot_count), x] = bf16(-(fine_sin * wc + fine_cos * ws))

    part[...] = jnp.zeros_like(part)
    ptb_in.wait()
    for hq in range(HALVES * QUADS):
        pltpu.make_async_copy(sbuf.at[hq, 0], gbuf.at[hq, 0], own_sem).wait()

    def arrived(hq, b):
        lo, n = ((0, 32), (32, 16))[b]
        got = gbuf.at[hq, pl.ds(0, row_count - 1), pl.ds(lo, n)]
        pltpu.make_async_copy(got, got, ar_sem.at[hq * 2 + b]).wait()

    upper = iota((row_count, 2 * quad, LANES), 1) >= quad

    def zonal_step(t, carry):
        h, b = t // 3, t % 3

        @pl.when(t == 0)
        def _():
            for hq in range(2):
                arrived(hq, 0)
                arrived(hq, 1)

        @pl.when(t == 3)
        def _():
            arrived(2, 0)
            arrived(3, 0)

        @pl.when(t == 5)
        def _():
            arrived(2, 1)
            arrived(3, 1)

        tile = pl.ds(pl.multiple_of(b * 16, 16), 16)
        first = f32(gbuf[h * QUADS, :, tile, :])
        second = f32(gbuf[h * QUADS + 1, :, tile, :])
        blocks = []
        for p in range(LATS // 2):
            u = first[:, p * 8 : p * 8 + 8]
            v = second[:, p * 8 : p * 8 + 8]
            for got in (
                jnp.where(upper, pltpu.roll(v, quad, 1), u),
                jnp.where(upper, v, pltpu.roll(u, quad, 1)),
            ):
                pair = bf16(got.reshape(row_count * slots, LANES)).T
                blocks.append(jnp.concatenate([pair[: LANES // 2], pair[LANES // 2 :]], axis=1))
        lhs = jnp.concatenate(blocks, axis=0)
        lats = pl.ds(b * LATS, LATS)
        for x in range(0, lon_count, PIECE):
            field = jnp.dot(lhs, basis[:, x : x + PIECE], preferred_element_type=jnp.float32)
            field = f32(bf16(field)).reshape(LATS, mem_count, taken, levels, PIECE)
            total = part[lats, :, x : x + PIECE]
            for i in range(mem_count):
                source = lax.rem(me + mem_count - i, mem_count)
                begin = source * members + h * taken
                near = f32(ptb[lats, pl.ds(begin, taken), :, x : x + PIECE])
                total += jnp.sum(field[:, i] * near, axis=1)
            part[lats, :, x : x + PIECE] = total
            out_ref[lats, :, x : x + PIECE] = bf16(total)
        return carry

    lax.fori_loop(0, HALVES * 3, zonal_step, 0)

    sent = sx.at[:, pl.ds(1, mem_count - 1)]
    pltpu.make_async_copy(sent, sent, xs_sem).wait()
    sent = sbuf.at[:, pl.ds(0, row_count - 1)]
    pltpu.make_async_copy(sent, sent, as_sem).wait()


def shards(control, vert_root, loc_spec, legendre, wave_table, lat_order, perturb):
    members, modes, parts, slots, totals = control.shape
    lat_count = legendre.shape[2]
    lats, _, levels, lon_count = perturb.shape
    row_count, mem_count = 64, 4
    taken = members // HALVES
    tall = taken * levels
    quad = slots // QUADS
    each = lats * quad
    size = slots * taken * modes
    small = pl.BlockSpec(memory_space=pltpu.VMEM)
    large = pl.BlockSpec(memory_space=pl.ANY)
    half = jnp.bfloat16
    return pl.pallas_call(
        kernel,
        out_shape=jax.ShapeDtypeStruct((lats, levels, lon_count), half),
        in_specs=[small, small, small, small, large, large, large],
        out_specs=small,
        scratch_shapes=[
            pltpu.VMEM(control.shape, half),
            pltpu.VMEM(legendre.shape, half),
            pltpu.VMEM(perturb.shape, half),
            pltpu.VMEM((size, size), half),
            pltpu.VMEM((lat_count, lat_count), half),
            pltpu.VMEM((HALVES, mem_count, slots, parts, tall, totals), half),
            pltpu.VMEM((HALVES, mem_count, slots, parts, tall, totals), half),
            pltpu.VMEM((lat_count * quad, LANES), jnp.float32),
            pltpu.VMEM((HALVES * QUADS, row_count, each, LANES), half),
            pltpu.VMEM((HALVES * QUADS, row_count, each, LANES), half),
            pltpu.VMEM((2 * row_count * slots, lon_count), half),
            pltpu.VMEM((lats, levels, lon_count), jnp.float32),
            pltpu.SemaphoreType.DMA((4,)),
            pltpu.SemaphoreType.DMA,
            pltpu.SemaphoreType.DMA((HALVES * QUADS,)),
            pltpu.SemaphoreType.DMA,
            pltpu.SemaphoreType.DMA((HALVES * QUADS * 2,)),
            pltpu.SemaphoreType.DMA,
        ],
        compiler_params=pltpu.CompilerParams(
            collective_id=0, has_side_effects=True, vmem_limit_bytes=VMEM_LIMIT
        ),
    )(
        vert_root,
        loc_spec[None],
        lat_order[None],
        wave_table[None],
        control,
        legendre,
        perturb,
    )


def solution(mesh):
    return jax.shard_map(
        shards,
        mesh=mesh,
        in_specs=(
            P("mem", None, None, "rows", None),
            P(),
            P(),
            P("rows", None, None),
            P(),
            P(),
            P("rows", None, "mem", None),
        ),
        out_specs=P("rows", "mem", None),
        check_vma=False,
    )
```

```python
import functools
import math

import jax
import jax.numpy as jnp
from jax import lax
from jax.experimental import pallas as pl
from jax.experimental.pallas import tpu as pltpu
from jax.sharding import PartitionSpec as P

HALVES = 2
QUADS = 2
LATS = 4
LANES = 128
PIECE = 512
OWN, SIDES, FAR = 0, 1, 3
CHUNKS = 4
PARTS = ((0, 48), (0, 48), (0, 48), (0, 32), (32, 16))
VMEM_LIMIT = 60 * 1024 * 1024
MESH = pl.DeviceIdType.MESH
Z, Y, CORES = 8, 4, 2


def f32(x):
    return x.astype(jnp.float32)


def bf16(x):
    return x.astype(jnp.bfloat16)


def iota(shape, dim):
    return lax.broadcasted_iota(jnp.int32, shape, dim)


def turn(at, by, count):
    return lax.rem(at + by, count)


def unweave(x, slots):
    half, both = x.shape[0] // 2, x.shape[1]
    upper = iota((half, both, x.shape[2]), 1) >= slots
    near, far = x[:half], x[half:]
    first = jnp.where(upper, pltpu.roll(far, slots, 1), near)
    second = jnp.where(upper, far, pltpu.roll(near, slots, 1))
    return [v.reshape(half * both, x.shape[2]) for v in (first, second)]


def kernel(
    root_ref, loc_ref, order_ref, wave_ref, ctl_hbm, leg_hbm, ptb_hbm, out_ref,
    ctl, leg, ptb, kron, onehot, sx, rx, stage, sbuf, gbuf, basis, total,
    load_sem, xs_sem, xr_sem, as_sem, ar_sem, own_sem,
):
    rows = lax.axis_index("rows")
    me = lax.axis_index("mem")
    mem_count, row_count = 4, 64
    members, modes, _, slots, totals = ctl.shape
    taken = members // HALVES
    levels = modes // mem_count
    lat_count = leg.shape[2]
    quad = slots // QUADS
    tall = taken * levels
    lats = lat_count // row_count

    ctl_in = [
        pltpu.make_async_copy(
            ctl_hbm.at[pl.ds(h * taken, taken)], ctl.at[pl.ds(h * taken, taken)], load_sem.at[h]
        )
        for h in range(HALVES)
    ]
    leg_in = pltpu.make_async_copy(leg_hbm, leg, load_sem.at[2])
    ptb_in = pltpu.make_async_copy(ptb_hbm, ptb, load_sem.at[3])
    for c in ctl_in:
        c.start()
    leg_in.start()

    barrier = pltpu.get_barrier_semaphore()
    z, y, core = rows // (Y * CORES), (rows // CORES) % Y, rows % CORES
    spots = [
        turn(y, w // CORES + 1, Y) * CORES + turn(core, w + 1, CORES) for w in range(Y * CORES)
    ]

    def each_peer(act):
        def plane(k, carry):
            dz = Z // 2 + (1 - 2 * (k % 2)) * ((k + 1) // 2)
            base = turn(z, dz, Z) * (Y * CORES)
            for spot in spots:
                act(base + spot)
            return carry

        lax.fori_loop(0, Z - 1, plane, 0)
        for spot in spots[:-1]:
            act(z * (Y * CORES) + spot)

    def greet(dest):
        pl.semaphore_signal(barrier, inc=1, device_id=(dest, me), device_id_type=MESH)

    each_peer(greet)
    for i in range(1, mem_count):
        pl.semaphore_signal(
            barrier, inc=1, device_id=(rows, turn(me, i, mem_count)), device_id_type=MESH
        )

    size = slots * taken * modes
    row, col = iota((size, modes), 0), iota((size, modes), 1)
    level = lax.rem(me + row // (slots * tall), mem_count) * levels + row % levels
    pick = bf16(f32(level == col))
    spread = bf16(f32(iota((modes, size), 0) == (iota((modes, size), 1) // slots) % modes))
    wide = jnp.dot(pick, bf16(root_ref[...]), preferred_element_type=jnp.float32)
    wide = jnp.dot(bf16(wide), spread, preferred_element_type=jnp.float32)
    row, col = iota((size, size), 0), iota((size, size), 1)
    same = ((row // tall) % slots == col % slots) & ((row // levels) % taken == col // (modes * slots))
    kron[...] = bf16(jnp.where(same, wide, 0.0))
    onehot[...] = bf16(f32(iota((lat_count, lat_count), 0) == order_ref[...])).T

    def spectra(h, first, count):
        width = slots * tall
        for r in range(2):
            x = f32(ctl[h * taken : (h + 1) * taken, :, r])
            x = bf16(x.reshape(taken * modes * slots, totals))
            some = kron[first * width : (first + count) * width]
            spec = jnp.dot(some, x, preferred_element_type=jnp.float32) * loc_ref[...]
            spec = bf16(spec).reshape(count, slots, tall, totals)
            sx[first : first + count, :, r, h * tall : (h + 1) * tall] = spec

    def exchange(q, i):
        part_of = pl.ds(q * quad, quad)
        return pltpu.make_async_remote_copy(
            src_ref=sx.at[i, part_of],
            dst_ref=rx.at[i, part_of],
            send_sem=xs_sem,
            recv_sem=xr_sem.at[2 if i == 2 else q],
            device_id=(rows, turn(me, i, mem_count)),
            device_id_type=MESH,
        )

    def push(part, chunk):
        lo, n = PARTS[part]

        def send(dest):
            pltpu.make_async_remote_copy(
                src_ref=sbuf.at[chunk, dest, pl.ds(lo, n)],
                dst_ref=gbuf.at[chunk, rows, pl.ds(lo, n)],
                send_sem=as_sem,
                recv_sem=ar_sem.at[part if isinstance(chunk, int) else chunk],
                device_id=(dest, me),
                device_id_type=MESH,
            ).start()

        each_peer(send)

    def stored(s, four):
        stage[pl.ds(s, lat_count, stride=quad), :] = lax.dot_general(
            onehot[...], bf16(four), (((1,), (1,)), ((), ())), preferred_element_type=jnp.float32
        )

    def keep(chunk):
        sbuf[chunk] = bf16(stage[...]).reshape(row_count, lats * quad, LANES)
        pltpu.make_async_copy(sbuf.at[chunk, rows], gbuf.at[chunk, rows], own_sem).start()

    def legendre_packed(chunk, spec, i):
        for s in range(quad):
            four = [
                jnp.dot(
                    spec[i, q * quad + s].reshape(2 * members * levels, totals),
                    leg[q * quad + s],
                    preferred_element_type=jnp.float32,
                )
                for q in range(QUADS)
            ]
            stored(s, jnp.concatenate(four, axis=0))
        keep(chunk)

    def legendre_sides(q, carry):
        got = rx.at[1, pl.ds(0, slots)]
        pltpu.make_async_copy(got, got, xr_sem.at[q]).wait()
        for s in range(quad):
            x = jnp.concatenate(
                [rx[i, q * quad + s, r] for r in range(2) for i in (1, 3)], axis=0
            )
            stored(s, jnp.dot(x, leg[q * quad + s], preferred_element_type=jnp.float32))
        keep(SIDES + q)
        push(SIDES, SIDES + q)
        return carry

    for h in range(HALVES):
        ctl_in[h].wait()
        spectra(h, 0, 1)
    leg_in.wait()
    legendre_packed(OWN, sx, 0)
    pl.semaphore_wait(barrier, row_count + mem_count - 2)
    push(OWN, OWN)
    for h in range(HALVES):
        spectra(h, 1, mem_count - 1)
    for i in (1, 3):
        exchange(0, i).start()
    for i in (1, 3):
        exchange(1, i).start()
    for q in range(QUADS):
        exchange(q, 2).start()
    ptb_in.start()

    slot_count, lon_count = basis.shape[0] // 2, basis.shape[1]
    wave = jnp.broadcast_to(wave_ref[...], (LANES, slot_count)).T
    waves = unweave(wave.reshape(row_count, slots, LANES), quad)
    some = slot_count // QUADS
    turns = lon_count // LANES
    for q, wave in enumerate(waves):
        weight = jnp.where(wave == 0, 1.0, 2.0)
        angle = f32(lax.rem(wave * iota(wave.shape, 1), lon_count)) * (2.0 * math.pi / lon_count)
        fine_cos, fine_sin = weight * jnp.cos(angle), weight * jnp.sin(angle)
        angle = f32(lax.rem(wave * iota(wave.shape, 1), turns)) * (2.0 * math.pi / turns)
        wide_cos, wide_sin = jnp.cos(angle), jnp.sin(angle)
        for a in range(turns):
            x = pl.ds(a * LANES, LANES)
            wc = wide_cos[:, a : a + 1]
            ws = wide_sin[:, a : a + 1]
            basis[pl.ds(2 * q * some, some), x] = bf16(fine_cos * wc - fine_sin * ws)
            basis[pl.ds((2 * q + 1) * some, some), x] = bf16(-(fine_sin * wc + fine_cos * ws))
    total[...] = jnp.zeros_like(total)

    lax.fori_loop(0, QUADS, legendre_sides, 0)
    got = rx.at[2]
    pltpu.make_async_copy(got, got, xr_sem.at[2]).wait()
    legendre_packed(FAR, rx, 2)
    push(3, FAR)
    push(4, FAR)

    ptb_in.wait()
    pltpu.make_async_copy(sbuf.at[:, 0], gbuf.at[:, 0], own_sem).wait()

    def arrived(part, chunk):
        lo, n = PARTS[part]
        got = gbuf.at[chunk, pl.ds(0, row_count - 1), pl.ds(lo, n)]
        pltpu.make_async_copy(got, got, ar_sem.at[part]).wait()

    def turned(chunk, b):
        tile = pl.ds(pl.multiple_of(b * 16, 16), 16)
        got = f32(gbuf[chunk, :, tile, :])
        return [
            bf16(v).T for p in range(LATS // 2) for v in unweave(got[:, p * 8 : p * 8 + 8], quad)
        ]

    def cut(x, count):
        n = LANES // count
        return [x[c * n : (c + 1) * n] for c in range(count)]

    def zonal(b, blocks, offsets):
        lhs = jnp.concatenate([jnp.concatenate(parts, axis=1) for parts in blocks], axis=0)
        here = pl.ds(b * LATS, LATS)
        for x in range(0, lon_count, PIECE):
            field = jnp.dot(lhs, basis[:, x : x + PIECE], preferred_element_type=jnp.float32)
            field = f32(bf16(field)).reshape(LATS, len(offsets), members, levels, PIECE)
            sums = total[here, :, x : x + PIECE]
            for n, i in enumerate(offsets):
                begin = turn(me, mem_count - i, mem_count) * members
                near = f32(ptb[here, pl.ds(begin, members), :, x : x + PIECE])
                sums += jnp.sum(field[:, n] * near, axis=1)
            total[here, :, x : x + PIECE] = sums
            if offsets == (2,):
                out_ref[here, :, x : x + PIECE] = bf16(sums)

    def own_step(b, carry):
        zonal(b, [cut(t, 2 * QUADS) for t in turned(OWN, b)], (0,))
        return carry

    def sides_step(b, carry):
        pairs = zip(turned(SIDES, b), turned(SIDES + 1, b))
        zonal(b, [cut(t, 2) + cut(u, 2) for t, u in pairs], (1, 3))
        return carry

    def far_step(b, carry):
        @pl.when(b == 2)
        def _():
            arrived(4, FAR)

        zonal(b, [cut(t, 2 * QUADS) for t in turned(FAR, b)], (2,))
        return carry

    arrived(0, OWN)
    lax.fori_loop(0, lats // LATS, own_step, 0)
    arrived(1, SIDES)
    arrived(2, SIDES + 1)
    lax.fori_loop(0, lats // LATS, sides_step, 0)
    arrived(3, FAR)
    lax.fori_loop(0, lats // LATS, far_step, 0)

    sent = sx.at[pl.ds(1, mem_count - 1)]
    pltpu.make_async_copy(sent, sent, xs_sem).wait()
    sent = sbuf.at[:, pl.ds(0, row_count - 1)]
    pltpu.make_async_copy(sent, sent, as_sem).wait()


def shards(control, vert_root, loc_spec, legendre, wave_table, lat_order, perturb):
    members, modes, parts, slots, totals = control.shape
    lat_count = legendre.shape[2]
    lats, _, levels, lon_count = perturb.shape
    row_count, mem_count = 64, 4
    quad = slots // QUADS
    each = lats * quad
    size = slots * (members // HALVES) * modes
    spectra = (mem_count, slots, parts, members * levels, totals)
    small = pl.BlockSpec(memory_space=pltpu.VMEM)
    large = pl.BlockSpec(memory_space=pl.ANY)
    half = jnp.bfloat16
    return pl.pallas_call(
        kernel,
        out_shape=jax.ShapeDtypeStruct((lats, levels, lon_count), half),
        in_specs=[small, small, small, small, large, large, large],
        out_specs=small,
        scratch_shapes=[
            pltpu.VMEM(control.shape, half),
            pltpu.VMEM(legendre.shape, half),
            pltpu.VMEM(perturb.shape, half),
            pltpu.VMEM((size, size), half),
            pltpu.VMEM((lat_count, lat_count), half),
            pltpu.VMEM(spectra, half),
            pltpu.VMEM(spectra, half),
            pltpu.VMEM((lat_count * quad, LANES), jnp.float32),
            pltpu.VMEM((CHUNKS, row_count, each, LANES), half),
            pltpu.VMEM((CHUNKS, row_count, each, LANES), half),
            pltpu.VMEM((2 * row_count * slots, lon_count), half),
            pltpu.VMEM((lats, levels, lon_count), jnp.float32),
            pltpu.SemaphoreType.DMA((4,)),
            pltpu.SemaphoreType.DMA,
            pltpu.SemaphoreType.DMA((3,)),
            pltpu.SemaphoreType.DMA,
            pltpu.SemaphoreType.DMA((5,)),
            pltpu.SemaphoreType.DMA,
        ],
        compiler_params=pltpu.CompilerParams(
            collective_id=0, has_side_effects=True, vmem_limit_bytes=VMEM_LIMIT
        ),
    )(
        vert_root,
        loc_spec[None],
        lat_order[None],
        wave_table[None],
        control,
        legendre,
        perturb,
    )


def solution(mesh):
    return jax.shard_map(
        shards,
        mesh=mesh,
        in_specs=(
            P("mem", None, None, "rows", None),
            P(),
            P(),
            P("rows", None, None),
            P(),
            P(),
            P("rows", None, "mem", None),
        ),
        out_specs=P("rows", "mem", None),
        check_vma=False,
    )
```

```python
import functools
import math

import jax
import jax.numpy as jnp
from jax import lax
from jax.experimental import pallas as pl
from jax.experimental.pallas import tpu as pltpu
from jax.sharding import PartitionSpec as P

HALVES = 2
QUADS = 2
LATS = 4
LANES = 128
PIECE = 512
OWN, SIDES, FAR = 0, 1, 3
CHUNKS = 4
PARTS = ((0, 48), (0, 48), (0, 48), (0, 32), (32, 16))
VMEM_LIMIT = 56 * 1024 * 1024
MESH = pl.DeviceIdType.MESH
Z, Y, CORES = 8, 4, 2


def f32(x):
    return x.astype(jnp.float32)


def bf16(x):
    return x.astype(jnp.bfloat16)


def iota(shape, dim):
    return lax.broadcasted_iota(jnp.int32, shape, dim)


def turn(at, by, count):
    return lax.rem(at + by, count)


def unweave(x, slots):
    half, both = x.shape[0] // 2, x.shape[1]
    upper = iota((half, both, x.shape[2]), 1) >= slots
    near, far = x[:half], x[half:]
    first = jnp.where(upper, pltpu.roll(far, slots, 1), near)
    second = jnp.where(upper, far, pltpu.roll(near, slots, 1))
    return [v.reshape(half * both, x.shape[2]) for v in (first, second)]


def kernel(
    root_hbm, loc_hbm, order_hbm, wave_hbm, ctl_hbm, leg_hbm, ptb_hbm, out_ref,
    root_ref, loc_ref, order_ref, wave_ref, ctl, leg, ptb, kron, onehot, sx, rx, stage, sbuf, gbuf, basis, total,
    load_sem, leg_sem, xs_sem, xr_sem, as_sem, ar_sem, own_sem,
):
    rows = lax.axis_index("rows")
    me = lax.axis_index("mem")
    mem_count, row_count = 4, 64
    members, modes, _, slots, totals = ctl.shape
    taken = members // HALVES
    levels = modes // mem_count
    lat_count = leg.shape[2]
    quad = slots // QUADS
    tall = taken * levels
    lats = lat_count // row_count

    ctl_in = [
        pltpu.make_async_copy(
            ctl_hbm.at[pl.ds(h * taken, taken)], ctl.at[pl.ds(h * taken, taken)], load_sem.at[h]
        )
        for h in range(HALVES)
    ]
    leg_in = [pltpu.make_async_copy(leg_hbm.at[s], leg.at[s], leg_sem.at[s]) for s in range(slots)]
    ptb_in = pltpu.make_async_copy(ptb_hbm, ptb, load_sem.at[2])
    root_in, loc_in, order_in, wave_in = [
        pltpu.make_async_copy(source, kept, load_sem.at[3 + n])
        for n, (source, kept) in enumerate(
            ((root_hbm, root_ref), (loc_hbm, loc_ref), (order_hbm, order_ref), (wave_hbm, wave_ref))
        )
    ]
    for c in (root_in, order_in, loc_in, *ctl_in, wave_in):
        c.start()

    for s in (0, 4, 1, 5):
        leg_in[s].start()

    barrier = pltpu.get_barrier_semaphore()
    z, y, core = rows // (Y * CORES), (rows // CORES) % Y, rows % CORES
    spots = [
        turn(y, w // CORES + 1, Y) * CORES + turn(core, w + 1, CORES) for w in range(Y * CORES)
    ]

    def each_peer(act):
        def plane(k, carry):
            dz = Z // 2 + (1 - 2 * (k % 2)) * ((k + 1) // 2)
            base = turn(z, dz, Z) * (Y * CORES)
            for spot in spots:
                act(base + spot)
            return carry

        lax.fori_loop(0, Z - 1, plane, 0)
        for spot in spots[:-1]:
            act(z * (Y * CORES) + spot)

    def greet(dest):
        pl.semaphore_signal(barrier, inc=1, device_id=(dest, me), device_id_type=MESH)

    each_peer(greet)
    for i in range(1, mem_count):
        pl.semaphore_signal(
            barrier, inc=1, device_id=(rows, turn(me, i, mem_count)), device_id_type=MESH
        )
    for s in (2, 3, 6, 7):
        leg_in[s].start()

    size = slots * taken * modes
    row, col = iota((size, modes), 0), iota((size, modes), 1)
    level = lax.rem(me + row // (slots * tall), mem_count) * levels + row % levels
    pick = bf16(f32(level == col))
    spread = bf16(f32(iota((modes, size), 0) == (iota((modes, size), 1) // slots) % modes))
    root_in.wait()
    wide = jnp.dot(pick, bf16(root_ref[...]), preferred_element_type=jnp.float32)
    wide = jnp.dot(bf16(wide), spread, preferred_element_type=jnp.float32)
    row, col = iota((size, size), 0), iota((size, size), 1)
    same = ((row // tall) % slots == col % slots) & ((row // levels) % taken == col // (modes * slots))
    kron[...] = bf16(jnp.where(same, wide, 0.0))

    def spectra(h, first, count):
        width = slots * tall
        for r in range(2):
            x = f32(ctl[h * taken : (h + 1) * taken, :, r])
            x = bf16(x.reshape(taken * modes * slots, totals))
            some = kron[first * width : (first + count) * width]
            spec = jnp.dot(some, x, preferred_element_type=jnp.float32) * loc_ref[...]
            spec = bf16(spec).reshape(count, slots, tall, totals)
            sx[first : first + count, :, r, h * tall : (h + 1) * tall] = spec

    def exchange(q, i):
        part_of = pl.ds(q * quad, quad)
        return pltpu.make_async_remote_copy(
            src_ref=sx.at[i, part_of],
            dst_ref=rx.at[i, part_of],
            send_sem=xs_sem,
            recv_sem=xr_sem.at[2 if i == 2 else q],
            device_id=(rows, turn(me, i, mem_count)),
            device_id_type=MESH,
        )

    def push(part, chunk):
        lo, n = PARTS[part]

        def send(dest):
            pltpu.make_async_remote_copy(
                src_ref=sbuf.at[chunk, dest, pl.ds(lo, n)],
                dst_ref=gbuf.at[chunk, rows, pl.ds(lo, n)],
                send_sem=as_sem,
                recv_sem=ar_sem.at[part if isinstance(chunk, int) else chunk],
                device_id=(dest, me),
                device_id_type=MESH,
            ).start()

        each_peer(send)

    def stored(s, four):
        stage[pl.ds(s, lat_count, stride=quad), :] = lax.dot_general(
            onehot[...], bf16(four), (((1,), (1,)), ((), ())), preferred_element_type=jnp.float32
        )

    def keep(chunk):
        sbuf[chunk] = bf16(stage[...]).reshape(row_count, lats * quad, LANES)
        pltpu.make_async_copy(sbuf.at[chunk, rows], gbuf.at[chunk, rows], own_sem).start()

    def legendre_packed(chunk, spec, i):
        for s in range(quad):
            if chunk == OWN and s % 2 == 0:
                for slot in (s, s + 1, s + quad, s + quad + 1):
                    leg_in[slot].wait()
            if chunk == OWN and s == 0:
                order = order_ref[...].reshape(1, lat_count)
                onehot[...] = bf16(f32(iota((lat_count, lat_count), 0) == order)).T
            four = []
            for slot in range(s, slots, quad):
                x = spec[i, slot].reshape(2 * members * levels, totals)
                four.append(jnp.dot(x, leg[slot], preferred_element_type=jnp.float32))
            stored(s, jnp.concatenate(four, axis=0))
        keep(chunk)

    def legendre_sides(q, carry):
        got = rx.at[1, pl.ds(0, slots)]
        pltpu.make_async_copy(got, got, xr_sem.at[q]).wait()
        for s in range(quad):
            x = jnp.concatenate(
                [rx[i, q * quad + s, r] for r in range(2) for i in (1, 3)], axis=0
            )
            stored(s, jnp.dot(x, leg[q * quad + s], preferred_element_type=jnp.float32))
        keep(SIDES + q)
        push(SIDES, SIDES + q)
        return carry

    order_in.wait()
    loc_in.wait()
    for h in range(HALVES):
        ctl_in[h].wait()
        spectra(h, 0, 1)
    legendre_packed(OWN, sx, 0)
    pl.semaphore_wait(barrier, row_count + mem_count - 2)
    push(OWN, OWN)
    for h in range(HALVES):
        spectra(h, 1, mem_count - 1)
    for i in (1, 3):
        exchange(0, i).start()
    for i in (1, 3):
        exchange(1, i).start()
    for q in range(QUADS):
        exchange(q, 2).start()
    ptb_in.start()

    slot_count, lon_count = basis.shape[0] // 2, basis.shape[1]
    wave_in.wait()
    wave = jnp.broadcast_to(wave_ref[...], (LANES, slot_count)).T
    waves = unweave(wave.reshape(row_count, slots, LANES), quad)
    some = slot_count // QUADS
    turns = lon_count // LANES
    for q, wave in enumerate(waves):
        weight = jnp.where(wave == 0, 1.0, 2.0)
        angle = f32(lax.rem(wave * iota(wave.shape, 1), lon_count)) * (2.0 * math.pi / lon_count)
        fine_cos, fine_sin = weight * jnp.cos(angle), weight * jnp.sin(angle)
        angle = f32(lax.rem(wave * iota(wave.shape, 1), turns)) * (2.0 * math.pi / turns)
        wide_cos, wide_sin = jnp.cos(angle), jnp.sin(angle)
        for a in range(turns):
            x = pl.ds(a * LANES, LANES)
            wc = wide_cos[:, a : a + 1]
            ws = wide_sin[:, a : a + 1]
            basis[pl.ds(2 * q * some, some), x] = bf16(fine_cos * wc - fine_sin * ws)
            basis[pl.ds((2 * q + 1) * some, some), x] = bf16(-(fine_sin * wc + fine_cos * ws))
    total[...] = jnp.zeros_like(total)

    lax.fori_loop(0, QUADS, legendre_sides, 0)
    got = rx.at[2]
    pltpu.make_async_copy(got, got, xr_sem.at[2]).wait()
    legendre_packed(FAR, rx, 2)
    push(3, FAR)
    push(4, FAR)

    ptb_in.wait()
    pltpu.make_async_copy(sbuf.at[:, 0], gbuf.at[:, 0], own_sem).wait()

    def arrived(part, chunk):
        lo, n = PARTS[part]
        got = gbuf.at[chunk, pl.ds(0, row_count - 1), pl.ds(lo, n)]
        pltpu.make_async_copy(got, got, ar_sem.at[part]).wait()

    def turned(chunk, b):
        tile = pl.ds(pl.multiple_of(b * 16, 16), 16)
        got = f32(gbuf[chunk, :, tile, :])
        return [
            bf16(v).T for p in range(LATS // 2) for v in unweave(got[:, p * 8 : p * 8 + 8], quad)
        ]

    def cut(x, count):
        n = LANES // count
        return [x[c * n : (c + 1) * n] for c in range(count)]

    def zonal(b, blocks, offsets):
        lhs = jnp.concatenate([jnp.concatenate(parts, axis=1) for parts in blocks], axis=0)
        here = pl.ds(b * LATS, LATS)
        for x in range(0, lon_count, PIECE):
            field = jnp.dot(lhs, basis[:, x : x + PIECE], preferred_element_type=jnp.float32)
            field = f32(bf16(field)).reshape(LATS, len(offsets), members, levels, PIECE)
            sums = total[here, :, x : x + PIECE]
            for n, i in enumerate(offsets):
                begin = turn(me, mem_count - i, mem_count) * members
                near = f32(ptb[here, pl.ds(begin, members), :, x : x + PIECE])
                sums += jnp.sum(field[:, n] * near, axis=1)
            total[here, :, x : x + PIECE] = sums
            if offsets == (2,):
                out_ref[here, :, x : x + PIECE] = bf16(sums)

    def own_step(b, carry):
        zonal(b, [cut(t, 2 * QUADS) for t in turned(OWN, b)], (0,))
        return carry

    def sides_step(b, carry):
        pairs = zip(turned(SIDES, b), turned(SIDES + 1, b))
        zonal(b, [cut(t, 2) + cut(u, 2) for t, u in pairs], (1, 3))
        return carry

    def far_step(b, carry):
        @pl.when(b == 2)
        def _():
            arrived(4, FAR)

        zonal(b, [cut(t, 2 * QUADS) for t in turned(FAR, b)], (2,))
        return carry

    arrived(0, OWN)
    lax.fori_loop(0, lats // LATS, own_step, 0)
    arrived(1, SIDES)
    arrived(2, SIDES + 1)
    lax.fori_loop(0, lats // LATS, sides_step, 0)
    arrived(3, FAR)
    lax.fori_loop(0, lats // LATS, far_step, 0)

    sent = sx.at[pl.ds(1, mem_count - 1)]
    pltpu.make_async_copy(sent, sent, xs_sem).wait()
    sent = sbuf.at[:, pl.ds(0, row_count - 1)]
    pltpu.make_async_copy(sent, sent, as_sem).wait()


def shards(control, vert_root, loc_spec, legendre, wave_table, lat_order, perturb):
    members, modes, parts, slots, totals = control.shape
    lat_count = legendre.shape[2]
    lats, _, levels, lon_count = perturb.shape
    row_count, mem_count = 64, 4
    quad = slots // QUADS
    each = lats * quad
    size = slots * (members // HALVES) * modes
    spectra = (mem_count, slots, parts, members * levels, totals)
    large = pl.BlockSpec(memory_space=pltpu.HBM)
    half = jnp.bfloat16
    return pl.pallas_call(
        kernel,
        out_shape=pltpu.VMEM((lats, levels, lon_count), half),
        in_specs=[large] * 7,
        out_specs=pl.BlockSpec(memory_space=pltpu.VMEM),
        scratch_shapes=[
            pltpu.VMEM(vert_root.shape, jnp.float32),
            pltpu.VMEM((1, totals), jnp.float32),
            pltpu.VMEM(lat_order.shape, jnp.int32),
            pltpu.VMEM((1, row_count * slots), jnp.int32),
            pltpu.VMEM(control.shape, half),
            pltpu.VMEM(legendre.shape, half),
            pltpu.VMEM(perturb.shape, half),
            pltpu.VMEM((size, size), half),
            pltpu.VMEM((lat_count, lat_count), half),
            pltpu.VMEM(spectra, half),
            pltpu.VMEM(spectra, half),
            pltpu.VMEM((lat_count * quad, LANES), jnp.float32),
            pltpu.VMEM((CHUNKS, row_count, each, LANES), half),
            pltpu.VMEM((CHUNKS, row_count, each, LANES), half),
            pltpu.VMEM((2 * row_count * slots, lon_count), half),
            pltpu.VMEM((lats, levels, lon_count), jnp.float32),
            pltpu.SemaphoreType.DMA((7,)),
            pltpu.SemaphoreType.DMA((slots,)),
            pltpu.SemaphoreType.DMA,
            pltpu.SemaphoreType.DMA((3,)),
            pltpu.SemaphoreType.DMA,
            pltpu.SemaphoreType.DMA((5,)),
            pltpu.SemaphoreType.DMA,
        ],
        compiler_params=pltpu.CompilerParams(
            collective_id=0, has_side_effects=True, vmem_limit_bytes=VMEM_LIMIT
        ),
    )(
        vert_root,
        loc_spec[None],
        lat_order,
        wave_table[None],
        control,
        legendre,
        perturb,
    )


def solution(mesh):
    return jax.shard_map(
        shards,
        mesh=mesh,
        in_specs=(
            P("mem", None, None, "rows", None),
            P(),
            P(),
            P("rows", None, None),
            P(),
            P(),
            P("rows", None, "mem", None),
        ),
        out_specs=P("rows", "mem", None),
        check_vma=False,
    )
```

```python
import functools
import math

import jax
import jax.numpy as jnp
from jax import lax
from jax.experimental import pallas as pl
from jax.experimental.pallas import tpu as pltpu
from jax.sharding import PartitionSpec as P

HALVES = 2
QUADS = 2
LATS = 4
LANES = 128
PIECE = 512
OWN, SIDES, FAR = 0, 1, 3
CHUNKS = 4
PARTS = ((0, 48), (0, 48), (0, 48), (0, 32), (32, 16))
VMEM_LIMIT = 56 * 1024 * 1024
MESH = pl.DeviceIdType.MESH
Z, Y, CORES = 8, 4, 2


def f32(x):
    return x.astype(jnp.float32)


def bf16(x):
    return x.astype(jnp.bfloat16)


def iota(shape, dim):
    return lax.broadcasted_iota(jnp.int32, shape, dim)


def turn(at, by, count):
    return lax.rem(at + by, count)


def unweave(x, slots):
    half, both = x.shape[0] // 2, x.shape[1]
    upper = iota((half, both, x.shape[2]), 1) >= slots
    near, far = x[:half], x[half:]
    first = jnp.where(upper, pltpu.roll(far, slots, 1), near)
    second = jnp.where(upper, far, pltpu.roll(near, slots, 1))
    return [v.reshape(half * both, x.shape[2]) for v in (first, second)]


def kernel(
    root_hbm, loc_hbm, order_hbm, wave_hbm, ctl_hbm, leg_hbm, ptb_hbm, out_ref,
    root_ref, loc_ref, order_ref, wave_ref, ctl, leg, ptb, kron, onehot, sx, rx, stage, sbuf, gbuf, basis, total,
    load_sem, leg_sem, xs_sem, xr_sem, as_sem, ar_sem, own_sem,
):
    rows = lax.axis_index("rows")
    me = lax.axis_index("mem")
    mem_count, row_count = 4, 64
    members, modes, _, slots, totals = ctl.shape
    taken = members // HALVES
    levels = modes // mem_count
    lat_count = leg.shape[2]
    quad = slots // QUADS
    tall = taken * levels
    lats = lat_count // row_count

    ctl_in = [
        pltpu.make_async_copy(
            ctl_hbm.at[pl.ds(h * taken, taken)], ctl.at[pl.ds(h * taken, taken)], load_sem.at[h]
        )
        for h in range(HALVES)
    ]
    leg_in = [pltpu.make_async_copy(leg_hbm.at[s], leg.at[s], leg_sem.at[s]) for s in range(slots)]
    ptb_in = pltpu.make_async_copy(ptb_hbm, ptb, load_sem.at[2])
    root_in, loc_in, order_in, wave_in = [
        pltpu.make_async_copy(source, kept, load_sem.at[3 + n])
        for n, (source, kept) in enumerate(
            ((root_hbm, root_ref), (loc_hbm, loc_ref), (order_hbm, order_ref), (wave_hbm, wave_ref))
        )
    ]
    for c in (root_in, order_in, loc_in, *ctl_in, wave_in):
        c.start()

    for s in (0, 4, 1, 5):
        leg_in[s].start()

    barrier = pltpu.get_barrier_semaphore()
    z, y, core = rows // (Y * CORES), (rows // CORES) % Y, rows % CORES
    spots = [
        turn(y, w // CORES + 1, Y) * CORES + turn(core, w + 1, CORES) for w in range(Y * CORES)
    ]

    def each_peer(act):
        def plane(k, carry):
            dz = Z // 2 + (1 - 2 * (k % 2)) * ((k + 1) // 2)
            base = turn(z, dz, Z) * (Y * CORES)
            for spot in spots:
                act(base + spot)
            return carry

        lax.fori_loop(0, Z - 1, plane, 0)
        for spot in spots[:-1]:
            act(z * (Y * CORES) + spot)

    def greet(dest):
        pl.semaphore_signal(barrier, inc=1, device_id=(dest, me), device_id_type=MESH)

    each_peer(greet)
    for i in range(1, mem_count):
        pl.semaphore_signal(
            barrier, inc=1, device_id=(rows, turn(me, i, mem_count)), device_id_type=MESH
        )
    for s in (2, 3, 6, 7):
        leg_in[s].start()

    size = slots * taken * modes
    row, col = iota((size, modes), 0), iota((size, modes), 1)
    level = lax.rem(me + row // (slots * tall), mem_count) * levels + row % levels
    pick = bf16(f32(level == col))
    spread = bf16(f32(iota((modes, size), 0) == (iota((modes, size), 1) // slots) % modes))
    root_in.wait()
    wide = jnp.dot(pick, bf16(root_ref[...]), preferred_element_type=jnp.float32)
    wide = jnp.dot(bf16(wide), spread, preferred_element_type=jnp.float32)
    row, col = iota((size, size), 0), iota((size, size), 1)
    same = ((row // tall) % slots == col % slots) & ((row // levels) % taken == col // (modes * slots))
    kron[...] = bf16(jnp.where(same, wide, 0.0))

    def spectra(h, first, count):
        width = slots * tall
        for r in range(2):
            x = f32(ctl[h * taken : (h + 1) * taken, :, r])
            x = bf16(x.reshape(taken * modes * slots, totals))
            some = kron[first * width : (first + count) * width]
            spec = jnp.dot(some, x, preferred_element_type=jnp.float32) * loc_ref[...]
            spec = bf16(spec).reshape(count, slots, tall, totals)
            sx[first : first + count, :, r, h * tall : (h + 1) * tall] = spec

    def exchange(q, i):
        part_of = pl.ds(q * quad, quad)
        return pltpu.make_async_remote_copy(
            src_ref=sx.at[i, part_of],
            dst_ref=rx.at[i, part_of],
            send_sem=xs_sem,
            recv_sem=xr_sem.at[2 if i == 2 else q],
            device_id=(rows, turn(me, i, mem_count)),
            device_id_type=MESH,
        )

    def push(part, chunk):
        lo, n = PARTS[part]

        def send(dest):
            pltpu.make_async_remote_copy(
                src_ref=sbuf.at[chunk, dest, pl.ds(lo, n)],
                dst_ref=gbuf.at[chunk, rows, pl.ds(lo, n)],
                send_sem=as_sem,
                recv_sem=ar_sem.at[part],
                device_id=(dest, me),
                device_id_type=MESH,
            ).start()

        each_peer(send)

    def stored(s, fours):
        rows_of = lax.dot_general(
            onehot[...],
            jnp.concatenate([bf16(f) for f in fours], axis=0),
            (((1,), (1,)), ((), ())),
            preferred_element_type=jnp.float32,
        )
        for n in range(2):
            stage[pl.ds(s + n, lat_count, stride=quad), :] = rows_of[:, n * LANES : (n + 1) * LANES]

    def keep(chunk):
        sbuf[chunk] = bf16(stage[...]).reshape(row_count, lats * quad, LANES)
        pltpu.make_async_copy(sbuf.at[chunk, rows], gbuf.at[chunk, rows], own_sem).start()

    def legendre_packed(chunk, spec, i):
        fours = []
        for s in range(0, quad, 2):
            if chunk == OWN:
                for slot in (s, s + 1, s + quad, s + quad + 1):
                    leg_in[slot].wait()
            if chunk == OWN and s == 0:
                order = order_ref[...].reshape(1, lat_count)
                onehot[...] = bf16(f32(iota((lat_count, lat_count), 0) == order)).T
            four = []
            for slot in (s, s + quad, s + 1, s + quad + 1):
                x = spec[i, slot].reshape(2 * members * levels, totals)
                four.append(bf16(jnp.dot(x, leg[slot], preferred_element_type=jnp.float32)))
            fours.append(four)
        for n, four in enumerate(fours):
            stored(2 * n, four)
        keep(chunk)

    def legendre_sides(q, carry):
        got = rx.at[1, pl.ds(0, slots)]
        pltpu.make_async_copy(got, got, xr_sem.at[q]).wait()
        for s in range(0, quad, 2):
            four = []
            for slot in (q * quad + s, q * quad + s + 1):
                x = jnp.concatenate([rx[i, slot, r] for r in range(2) for i in (1, 3)], axis=0)
                four.append(jnp.dot(x, leg[slot], preferred_element_type=jnp.float32))
            stored(s, four)
        keep(SIDES + q)
        return carry

    order_in.wait()
    loc_in.wait()
    for h in range(HALVES):
        ctl_in[h].wait()
        spectra(h, 0, 1)
    legendre_packed(OWN, sx, 0)
    pl.semaphore_wait(barrier, row_count + mem_count - 2)
    push(OWN, OWN)
    for h in range(HALVES):
        spectra(h, 1, mem_count - 1)
    for i in (1, 3):
        exchange(0, i).start()
    for i in (1, 3):
        exchange(1, i).start()
    for q in range(QUADS):
        exchange(q, 2).start()
    ptb_in.start()

    slot_count, lon_count = basis.shape[0] // 2, basis.shape[1]
    wave_in.wait()
    wave = jnp.broadcast_to(wave_ref[...], (LANES, slot_count)).T
    waves = unweave(wave.reshape(row_count, slots, LANES), quad)
    some = slot_count // QUADS
    turns = lon_count // LANES
    for q, wave in enumerate(waves):
        weight = jnp.where(wave == 0, 1.0, 2.0)
        angle = f32(lax.rem(wave * iota(wave.shape, 1), lon_count)) * (2.0 * math.pi / lon_count)
        fine_cos, fine_sin = weight * jnp.cos(angle), weight * jnp.sin(angle)
        angle = f32(lax.rem(wave * iota(wave.shape, 1), turns)) * (2.0 * math.pi / turns)
        wide_cos, wide_sin = jnp.cos(angle), jnp.sin(angle)
        for a in range(turns):
            x = pl.ds(a * LANES, LANES)
            wc = wide_cos[:, a : a + 1]
            ws = wide_sin[:, a : a + 1]
            basis[pl.ds(2 * q * some, some), x] = bf16(fine_cos * wc - fine_sin * ws)
            basis[pl.ds((2 * q + 1) * some, some), x] = bf16(-(fine_sin * wc + fine_cos * ws))
    total[...] = jnp.zeros_like(total)

    lax.fori_loop(0, QUADS, legendre_sides, 0)
    push(1, pl.ds(SIDES, QUADS))
    got = rx.at[2]
    pltpu.make_async_copy(got, got, xr_sem.at[2]).wait()
    legendre_packed(FAR, rx, 2)
    push(3, FAR)
    push(4, FAR)

    ptb_in.wait()
    pltpu.make_async_copy(sbuf.at[:, 0], gbuf.at[:, 0], own_sem).wait()

    def arrived(part, chunk):
        lo, n = PARTS[part]
        got = gbuf.at[chunk, pl.ds(0, row_count - 1), pl.ds(lo, n)]
        pltpu.make_async_copy(got, got, ar_sem.at[part]).wait()

    def turned(chunk, b):
        tile = pl.ds(pl.multiple_of(b * 16, 16), 16)
        got = f32(gbuf[chunk, :, tile, :])
        return [
            bf16(v).T for p in range(LATS // 2) for v in unweave(got[:, p * 8 : p * 8 + 8], quad)
        ]

    def cut(x, count):
        n = LANES // count
        return [x[c * n : (c + 1) * n] for c in range(count)]

    def zonal(b, blocks, offsets):
        lhs = jnp.concatenate([jnp.concatenate(parts, axis=1) for parts in blocks], axis=0)
        here = pl.ds(b * LATS, LATS)
        for x in range(0, lon_count, PIECE):
            field = jnp.dot(lhs, basis[:, x : x + PIECE], preferred_element_type=jnp.float32)
            field = f32(bf16(field)).reshape(LATS, len(offsets), members, levels, PIECE)
            sums = total[here, :, x : x + PIECE]
            for n, i in enumerate(offsets):
                begin = turn(me, mem_count - i, mem_count) * members
                near = f32(ptb[here, pl.ds(begin, members), :, x : x + PIECE])
                sums += jnp.sum(field[:, n] * near, axis=1)
            total[here, :, x : x + PIECE] = sums
            if offsets == (2,):
                out_ref[here, :, x : x + PIECE] = bf16(sums)

    def own_step(b, carry):
        zonal(b, [cut(t, 2 * QUADS) for t in turned(OWN, b)], (0,))
        return carry

    def sides_step(b, carry):
        pairs = zip(turned(SIDES, b), turned(SIDES + 1, b))
        zonal(b, [cut(t, 2) + cut(u, 2) for t, u in pairs], (1, 3))
        return carry

    def far_step(b, carry):
        @pl.when(b == 2)
        def _():
            arrived(4, FAR)

        zonal(b, [cut(t, 2 * QUADS) for t in turned(FAR, b)], (2,))
        return carry

    arrived(0, OWN)
    lax.fori_loop(0, lats // LATS, own_step, 0)
    arrived(1, pl.ds(SIDES, QUADS))
    lax.fori_loop(0, lats // LATS, sides_step, 0)
    arrived(3, FAR)
    lax.fori_loop(0, lats // LATS, far_step, 0)

    sent = sx.at[pl.ds(1, mem_count - 1)]
    pltpu.make_async_copy(sent, sent, xs_sem).wait()
    sent = sbuf.at[:, pl.ds(0, row_count - 1)]
    pltpu.make_async_copy(sent, sent, as_sem).wait()


def shards(control, vert_root, loc_spec, legendre, wave_table, lat_order, perturb):
    members, modes, parts, slots, totals = control.shape
    lat_count = legendre.shape[2]
    lats, _, levels, lon_count = perturb.shape
    row_count, mem_count = 64, 4
    quad = slots // QUADS
    each = lats * quad
    size = slots * (members // HALVES) * modes
    spectra = (mem_count, slots, parts, members * levels, totals)
    large = pl.BlockSpec(memory_space=pltpu.HBM)
    half = jnp.bfloat16
    return pl.pallas_call(
        kernel,
        out_shape=pltpu.VMEM((lats, levels, lon_count), half),
        in_specs=[large] * 7,
        out_specs=pl.BlockSpec(memory_space=pltpu.VMEM),
        scratch_shapes=[
            pltpu.VMEM(vert_root.shape, jnp.float32),
            pltpu.VMEM((1, totals), jnp.float32),
            pltpu.VMEM(lat_order.shape, jnp.int32),
            pltpu.VMEM((1, row_count * slots), jnp.int32),
            pltpu.VMEM(control.shape, half),
            pltpu.VMEM(legendre.shape, half),
            pltpu.VMEM(perturb.shape, half),
            pltpu.VMEM((size, size), half),
            pltpu.VMEM((lat_count, lat_count), half),
            pltpu.VMEM(spectra, half),
            pltpu.VMEM(spectra, half),
            pltpu.VMEM((lat_count * quad, LANES), jnp.float32),
            pltpu.VMEM((CHUNKS, row_count, each, LANES), half),
            pltpu.VMEM((CHUNKS, row_count, each, LANES), half),
            pltpu.VMEM((2 * row_count * slots, lon_count), half),
            pltpu.VMEM((lats, levels, lon_count), jnp.float32),
            pltpu.SemaphoreType.DMA((7,)),
            pltpu.SemaphoreType.DMA((slots,)),
            pltpu.SemaphoreType.DMA,
            pltpu.SemaphoreType.DMA((3,)),
            pltpu.SemaphoreType.DMA,
            pltpu.SemaphoreType.DMA((5,)),
            pltpu.SemaphoreType.DMA,
        ],
        compiler_params=pltpu.CompilerParams(
            collective_id=0, has_side_effects=True, vmem_limit_bytes=VMEM_LIMIT
        ),
    )(
        vert_root,
        loc_spec[None],
        lat_order,
        wave_table[None],
        control,
        legendre,
        perturb,
    )


def solution(mesh):
    return jax.shard_map(
        shards,
        mesh=mesh,
        in_specs=(
            P("mem", None, None, "rows", None),
            P(),
            P(),
            P("rows", None, None),
            P(),
            P(),
            P("rows", None, "mem", None),
        ),
        out_specs=P("rows", "mem", None),
        check_vma=False,
    )
```

```python
import functools
import math

import jax
import jax.numpy as jnp
from jax import lax
from jax.experimental import pallas as pl
from jax.experimental.pallas import tpu as pltpu
from jax.sharding import PartitionSpec as P

HALVES = 2
QUADS = 2
LATS = 4
LANES = 128
PIECE = 512
OWN, SIDES, FAR = 0, 1, 3
CHUNKS = 4
PARTS = ((0, 48), (0, 48), (0, 48), (0, 32), (32, 16))
VMEM_LIMIT = 56 * 1024 * 1024
MESH = pl.DeviceIdType.MESH
Z, Y, CORES = 8, 4, 2


def f32(x):
    return x.astype(jnp.float32)


def bf16(x):
    return x.astype(jnp.bfloat16)


def iota(shape, dim):
    return lax.broadcasted_iota(jnp.int32, shape, dim)


def turn(at, by, count):
    return lax.rem(at + by, count)


def unweave(x, slots):
    half, both = x.shape[0] // 2, x.shape[1]
    upper = iota((half, both, x.shape[2]), 1) >= slots
    near, far = x[:half], x[half:]
    first = jnp.where(upper, pltpu.roll(far, slots, 1), near)
    second = jnp.where(upper, far, pltpu.roll(near, slots, 1))
    return [v.reshape(half * both, x.shape[2]) for v in (first, second)]


def kernel(
    root_hbm, loc_hbm, order_hbm, wave_hbm, ctl_hbm, leg_hbm, ptb_hbm, out_ref,
    root_ref, loc_ref, order_ref, wave_ref, ctl, leg, ptb, kron, onehot, sx, rx, stage, sbuf, gbuf, basis, total,
    load_sem, leg_sem, xs_sem, xr_sem, as_sem, ar_sem, own_sem,
):
    rows = lax.axis_index("rows")
    me = lax.axis_index("mem")
    mem_count, row_count = 4, 64
    members, modes, _, slots, totals = ctl.shape
    taken = members // HALVES
    levels = modes // mem_count
    lat_count = leg.shape[2]
    quad = slots // QUADS
    tall = taken * levels
    lats = lat_count // row_count

    ctl_in = [
        pltpu.make_async_copy(
            ctl_hbm.at[pl.ds(h * taken, taken)], ctl.at[pl.ds(h * taken, taken)], load_sem.at[h]
        )
        for h in range(HALVES)
    ]
    leg_in = [pltpu.make_async_copy(leg_hbm.at[s], leg.at[s], leg_sem.at[s]) for s in range(slots)]
    ptb_in = pltpu.make_async_copy(ptb_hbm, ptb, load_sem.at[2])
    root_in, loc_in, order_in, wave_in = [
        pltpu.make_async_copy(source, kept, load_sem.at[3 + n])
        for n, (source, kept) in enumerate(
            ((root_hbm, root_ref), (loc_hbm, loc_ref), (order_hbm, order_ref), (wave_hbm, wave_ref))
        )
    ]
    for c in (root_in, order_in, loc_in, *ctl_in, wave_in):
        c.start()

    for s in (0, 4, 1, 5):
        leg_in[s].start()

    barrier = pltpu.get_barrier_semaphore()
    z, y, core = rows // (Y * CORES), (rows // CORES) % Y, rows % CORES
    spots = [
        turn(y, dy, Y) * CORES + turn(core, dc, CORES) for dy in (2, 1, 3, 0) for dc in (1, 0)
    ]

    def each_peer(act):
        def plane(k, carry):
            dz = Z // 2 + (1 - 2 * (k % 2)) * ((k + 1) // 2)
            base = turn(z, dz, Z) * (Y * CORES)
            for spot in spots:
                act(base + spot)
            return carry

        lax.fori_loop(0, Z - 1, plane, 0)
        for spot in spots[:-1]:
            act(z * (Y * CORES) + spot)

    def greet(dest):
        pl.semaphore_signal(barrier, inc=1, device_id=(dest, me), device_id_type=MESH)

    each_peer(greet)
    for i in range(1, mem_count):
        pl.semaphore_signal(
            barrier, inc=1, device_id=(rows, turn(me, i, mem_count)), device_id_type=MESH
        )
    for s in (2, 3, 6, 7):
        leg_in[s].start()

    size = slots * taken * modes
    row, col = iota((size, modes), 0), iota((size, modes), 1)
    level = lax.rem(me + row // (slots * tall), mem_count) * levels + row % levels
    pick = bf16(f32(level == col))
    spread = bf16(f32(iota((modes, size), 0) == (iota((modes, size), 1) // slots) % modes))
    root_in.wait()
    wide = jnp.dot(pick, bf16(root_ref[...]), preferred_element_type=jnp.float32)
    wide = jnp.dot(bf16(wide), spread, preferred_element_type=jnp.float32)
    row, col = iota((size, size), 0), iota((size, size), 1)
    same = ((row // tall) % slots == col % slots) & ((row // levels) % taken == col // (modes * slots))
    kron[...] = bf16(jnp.where(same, wide, 0.0))

    def spectra(h, first, count):
        width = slots * tall
        for r in range(2):
            x = f32(ctl[h * taken : (h + 1) * taken, :, r])
            x = bf16(x.reshape(taken * modes * slots, totals))
            some = kron[first * width : (first + count) * width]
            spec = jnp.dot(some, x, preferred_element_type=jnp.float32) * loc_ref[...]
            spec = bf16(spec).reshape(count, slots, tall, totals)
            sx[first : first + count, :, r, h * tall : (h + 1) * tall] = spec

    def exchange(q, i):
        part_of = pl.ds(q * quad, quad)
        return pltpu.make_async_remote_copy(
            src_ref=sx.at[i, part_of],
            dst_ref=rx.at[i, part_of],
            send_sem=xs_sem,
            recv_sem=xr_sem.at[2 if i == 2 else q],
            device_id=(rows, turn(me, i, mem_count)),
            device_id_type=MESH,
        )

    def push(part, chunk):
        lo, n = PARTS[part]

        def send(dest):
            pltpu.make_async_remote_copy(
                src_ref=sbuf.at[chunk, dest, pl.ds(lo, n)],
                dst_ref=gbuf.at[chunk, rows, pl.ds(lo, n)],
                send_sem=as_sem,
                recv_sem=ar_sem.at[part],
                device_id=(dest, me),
                device_id_type=MESH,
            ).start()

        each_peer(send)

    def stored(s, fours):
        rows_of = lax.dot_general(
            onehot[...],
            jnp.concatenate([bf16(f) for f in fours], axis=0),
            (((1,), (1,)), ((), ())),
            preferred_element_type=jnp.float32,
        )
        for n in range(2):
            stage[pl.ds(s + n, lat_count, stride=quad), :] = rows_of[:, n * LANES : (n + 1) * LANES]

    def keep(chunk):
        sbuf[chunk] = bf16(stage[...]).reshape(row_count, lats * quad, LANES)
        pltpu.make_async_copy(sbuf.at[chunk, rows], gbuf.at[chunk, rows], own_sem).start()

    def legendre_packed(chunk, spec, i):
        fours = []
        for s in range(0, quad, 2):
            if chunk == OWN:
                for slot in (s, s + 1, s + quad, s + quad + 1):
                    leg_in[slot].wait()
            if chunk == OWN and s == 0:
                order = order_ref[...].reshape(1, lat_count)
                onehot[...] = bf16(f32(iota((lat_count, lat_count), 0) == order)).T
            four = []
            for slot in (s, s + quad, s + 1, s + quad + 1):
                x = spec[i, slot].reshape(2 * members * levels, totals)
                four.append(bf16(jnp.dot(x, leg[slot], preferred_element_type=jnp.float32)))
            fours.append(four)
        for n, four in enumerate(fours):
            stored(2 * n, four)
        keep(chunk)

    def legendre_sides(q, carry):
        got = rx.at[1, pl.ds(0, slots)]
        pltpu.make_async_copy(got, got, xr_sem.at[q]).wait()
        for s in range(0, quad, 2):
            four = []
            for slot in (q * quad + s, q * quad + s + 1):
                x = jnp.concatenate([rx[i, slot, r] for r in range(2) for i in (1, 3)], axis=0)
                four.append(jnp.dot(x, leg[slot], preferred_element_type=jnp.float32))
            stored(s, four)
        keep(SIDES + q)
        return carry

    order_in.wait()
    loc_in.wait()
    for h in range(HALVES):
        ctl_in[h].wait()
        spectra(h, 0, 1)
    legendre_packed(OWN, sx, 0)
    pl.semaphore_wait(barrier, row_count + mem_count - 2)
    push(OWN, OWN)
    for h in range(HALVES):
        spectra(h, 1, mem_count - 1)
    for i in (1, 3):
        exchange(0, i).start()
    for i in (1, 3):
        exchange(1, i).start()
    for q in range(QUADS):
        exchange(q, 2).start()
    ptb_in.start()

    slot_count, lon_count = basis.shape[0] // 2, basis.shape[1]
    wave_in.wait()
    wave = jnp.broadcast_to(wave_ref[...], (LANES, slot_count)).T
    waves = unweave(wave.reshape(row_count, slots, LANES), quad)
    some = slot_count // QUADS
    turns = lon_count // LANES
    for q, wave in enumerate(waves):
        weight = jnp.where(wave == 0, 1.0, 2.0)
        angle = f32(lax.rem(wave * iota(wave.shape, 1), lon_count)) * (2.0 * math.pi / lon_count)
        fine_cos, fine_sin = weight * jnp.cos(angle), weight * jnp.sin(angle)
        angle = f32(lax.rem(wave * iota(wave.shape, 1), turns)) * (2.0 * math.pi / turns)
        wide_cos, wide_sin = jnp.cos(angle), jnp.sin(angle)
        for a in range(turns):
            x = pl.ds(a * LANES, LANES)
            wc = wide_cos[:, a : a + 1]
            ws = wide_sin[:, a : a + 1]
            basis[pl.ds(2 * q * some, some), x] = bf16(fine_cos * wc - fine_sin * ws)
            basis[pl.ds((2 * q + 1) * some, some), x] = bf16(-(fine_sin * wc + fine_cos * ws))
    total[...] = jnp.zeros_like(total)

    lax.fori_loop(0, QUADS, legendre_sides, 0)
    push(1, pl.ds(SIDES, QUADS))
    got = rx.at[2]
    pltpu.make_async_copy(got, got, xr_sem.at[2]).wait()
    legendre_packed(FAR, rx, 2)
    push(3, FAR)
    push(4, FAR)

    ptb_in.wait()
    pltpu.make_async_copy(sbuf.at[:, 0], gbuf.at[:, 0], own_sem).wait()

    def arrived(part, chunk):
        lo, n = PARTS[part]
        got = gbuf.at[chunk, pl.ds(0, row_count - 1), pl.ds(lo, n)]
        pltpu.make_async_copy(got, got, ar_sem.at[part]).wait()

    def turned(chunk, b):
        tile = pl.ds(pl.multiple_of(b * 16, 16), 16)
        got = f32(gbuf[chunk, :, tile, :])
        return [
            bf16(v).T for p in range(LATS // 2) for v in unweave(got[:, p * 8 : p * 8 + 8], quad)
        ]

    def cut(x, count):
        n = LANES // count
        return [x[c * n : (c + 1) * n] for c in range(count)]

    def zonal(b, blocks, offsets):
        lhs = jnp.concatenate([jnp.concatenate(parts, axis=1) for parts in blocks], axis=0)
        here = pl.ds(b * LATS, LATS)
        for x in range(0, lon_count, PIECE):
            field = jnp.dot(lhs, basis[:, x : x + PIECE], preferred_element_type=jnp.float32)
            field = f32(bf16(field)).reshape(LATS, len(offsets), members, levels, PIECE)
            sums = total[here, :, x : x + PIECE]
            for n, i in enumerate(offsets):
                begin = turn(me, mem_count - i, mem_count) * members
                near = f32(ptb[here, pl.ds(begin, members), :, x : x + PIECE])
                sums += jnp.sum(field[:, n] * near, axis=1)
            total[here, :, x : x + PIECE] = sums
            if offsets == (2,):
                out_ref[here, :, x : x + PIECE] = bf16(sums)

    def own_step(b, carry):
        zonal(b, [cut(t, 2 * QUADS) for t in turned(OWN, b)], (0,))
        return carry

    def sides_step(b, carry):
        pairs = zip(turned(SIDES, b), turned(SIDES + 1, b))
        zonal(b, [cut(t, 2) + cut(u, 2) for t, u in pairs], (1, 3))
        return carry

    def far_step(b, carry):
        @pl.when(b == 2)
        def _():
            arrived(4, FAR)

        zonal(b, [cut(t, 2 * QUADS) for t in turned(FAR, b)], (2,))
        return carry

    arrived(0, OWN)
    lax.fori_loop(0, lats // LATS, own_step, 0)
    arrived(1, pl.ds(SIDES, QUADS))
    lax.fori_loop(0, lats // LATS, sides_step, 0)
    arrived(3, FAR)
    lax.fori_loop(0, lats // LATS, far_step, 0)

    sent = sx.at[pl.ds(1, mem_count - 1)]
    pltpu.make_async_copy(sent, sent, xs_sem).wait()
    sent = sbuf.at[:, pl.ds(0, row_count - 1)]
    pltpu.make_async_copy(sent, sent, as_sem).wait()


def shards(control, vert_root, loc_spec, legendre, wave_table, lat_order, perturb):
    members, modes, parts, slots, totals = control.shape
    lat_count = legendre.shape[2]
    lats, _, levels, lon_count = perturb.shape
    row_count, mem_count = 64, 4
    quad = slots // QUADS
    each = lats * quad
    size = slots * (members // HALVES) * modes
    spectra = (mem_count, slots, parts, members * levels, totals)
    large = pl.BlockSpec(memory_space=pltpu.HBM)
    half = jnp.bfloat16
    return pl.pallas_call(
        kernel,
        out_shape=pltpu.VMEM((lats, levels, lon_count), half),
        in_specs=[large] * 7,
        out_specs=pl.BlockSpec(memory_space=pltpu.VMEM),
        scratch_shapes=[
            pltpu.VMEM(vert_root.shape, jnp.float32),
            pltpu.VMEM((1, totals), jnp.float32),
            pltpu.VMEM(lat_order.shape, jnp.int32),
            pltpu.VMEM((1, row_count * slots), jnp.int32),
            pltpu.VMEM(control.shape, half),
            pltpu.VMEM(legendre.shape, half),
            pltpu.VMEM(perturb.shape, half),
            pltpu.VMEM((size, size), half),
            pltpu.VMEM((lat_count, lat_count), half),
            pltpu.VMEM(spectra, half),
            pltpu.VMEM(spectra, half),
            pltpu.VMEM((lat_count * quad, LANES), jnp.float32),
            pltpu.VMEM((CHUNKS, row_count, each, LANES), half),
            pltpu.VMEM((CHUNKS, row_count, each, LANES), half),
            pltpu.VMEM((2 * row_count * slots, lon_count), half),
            pltpu.VMEM((lats, levels, lon_count), jnp.float32),
            pltpu.SemaphoreType.DMA((7,)),
            pltpu.SemaphoreType.DMA((slots,)),
            pltpu.SemaphoreType.DMA,
            pltpu.SemaphoreType.DMA((3,)),
            pltpu.SemaphoreType.DMA,
            pltpu.SemaphoreType.DMA((5,)),
            pltpu.SemaphoreType.DMA,
        ],
        compiler_params=pltpu.CompilerParams(
            collective_id=0, has_side_effects=True, vmem_limit_bytes=VMEM_LIMIT
        ),
    )(
        vert_root,
        loc_spec[None],
        lat_order,
        wave_table[None],
        control,
        legendre,
        perturb,
    )


def solution(mesh):
    return jax.shard_map(
        shards,
        mesh=mesh,
        in_specs=(
            P("mem", None, None, "rows", None),
            P(),
            P(),
            P("rows", None, None),
            P(),
            P(),
            P("rows", None, "mem", None),
        ),
        out_specs=P("rows", "mem", None),
        check_vma=False,
    )
```
